256 devices in a mesh: blk: 16 (over z, y_lo), tp: 4 (over x), qg: 4 (over y_hi, core).
Axes of the slice: x: 4, y: 4 (y_hi: 2, y_lo: 2; y = y_hi * 2 + y_lo), z: 8, core: 2. Of those that a mesh axis runs over, the one named last changes fastest.
Arguments:
- hidden_states: bfloat16 [12288, 4096], P(('blk', 'tp'), 'qg'), may hold values from -8 to 8
- query_states: bfloat16 [256, 4096], P('tp', 'qg'), may hold values from -8 to 8
- w_query: bfloat16 [4096, 4096], P('qg', 'tp'), may hold values from -0.25 to 0.25
- w_key: bfloat16 [4096, 1024], P('qg', 'tp'), may hold values from -0.09375 to 0.09375
- w_value: bfloat16 [4096, 1024], P('qg', 'tp'), may hold values from -0.09375 to 0.09375
- slot_order: int32 [32], replicated, may hold values from 0 to 31, each once
Outputs:
- attention: bfloat16 [12288, 4096], P(('blk', 'qg'), 'tp')
- decoded: bfloat16 [256, 4096], P('qg', 'tp')
The draws below stay inside these ranges and needn't reach their ends.
Inputs may be any that keep to these rules, and one draw needn't show every extreme that they name: slot_order holds every number of 0 to 31 once.
All inputs are finite; a program needn't handle non-finite values.
Results may differ from the reference program's by a relative error of at most 0.00775.
The reference program's roundings to bfloat16 on the way count: a program that leaves them out, or rounds other values in their place, can miss the bound.
Values may be sent and summed in bfloat16 or wider, within the bound.
No kernel may reach another device: no remote copies, remote signals or barrier semaphores. Data moves between devices by JAX's collectives and lax.ppermute only.
A program may use at most 128 MiB of HBM per device.

```python
import math
import jax
import jax.numpy as jnp
from jax import lax

D = 4096
HEADS = 32
KV_HEADS = 8
HEAD_DIM = 128
QUERIES = 256
SEQ = 12288
SPAN = 384
SLOTS = 32


def draw_rows(key, row_count, columns, period):
    base_key, pick_key, forced_key, sign_key, size_key = jax.random.split(key, 5)
    drawn = jax.random.normal(base_key, (row_count, columns), jnp.float32)
    return jnp.clip(drawn, -8.0, 8.0).astype(jnp.bfloat16)


def draw_hidden_states(key, part):
    return draw_rows(jax.random.fold_in(key, 11), SEQ, D, 256)


def draw_query_states(key, part):
    return draw_rows(jax.random.fold_in(key, 23), QUERIES, D, 16)


def shard_levels(stream_key, extent, cuts, low, largest):
    def one(axis_at, blocks):
        heights = jax.random.uniform(jax.random.fold_in(jax.random.fold_in(stream_key, 6), axis_at), (blocks,), jnp.float32, low / len(cuts), largest / len(cuts))
        return jnp.repeat(jnp.exp(heights), extent[axis_at] // blocks).reshape((-1,) + (1,) * (len(extent) - axis_at - 1))

    gain = one(*cuts[0])
    for cut in cuts[1:]:
        gain = gain * one(*cut)
    return gain


def normal_values(own_key, shape, spread, most, pieces=(), kind=jnp.bfloat16):
    result = spread * jax.random.normal(own_key, shape, jnp.float32)
    if pieces:
        result = result * shard_levels(own_key, shape, pieces, -0.22, 0.18)
    return jnp.clip(result, -most, most).astype(kind)


def setup_inputs(seed: int = 0) -> dict:
    splits = jax.random.split(jax.random.key(seed), 7)
    hidden_states = draw_hidden_states(jax.random.fold_in(splits[6], 71), 0)
    query_states = draw_query_states(jax.random.fold_in(splits[6], 71), 0)
    w_query = normal_values(splits[2], (D, HEADS * HEAD_DIM), (D // 9) ** -0.5, 0.25, ((0, 4), (1, 4)))
    w_key = normal_values(splits[3], (D, KV_HEADS * HEAD_DIM), D ** -0.5, 0.09375, ((0, 4), (1, 4)))
    w_value = normal_values(splits[4], (D, KV_HEADS * HEAD_DIM), D ** -0.5, 0.09375, ((0, 4), (1, 4)))
    slot_order = jax.random.permutation(splits[5], SLOTS).astype(jnp.int32)
    return {"hidden_states": hidden_states, "query_states": query_states, "w_query": w_query, "w_key": w_key, "w_value": w_value, "slot_order": slot_order}


rope_base = 500000.0

def rotate(value_heads, position):
    full_dim = value_heads.shape[-1]
    half_dim = full_dim // 2
    frequency = jnp.float32(rope_base) ** (jnp.arange(half_dim, dtype=jnp.float32) * jnp.float32(-2.0 / full_dim))
    angles = position[:, None] * frequency[None, :]
    cosine = jnp.cos(angles)[:, None, :]
    sine_table = jnp.sin(angles)[:, None, :]
    front_half = value_heads[..., :half_dim]
    back_half = value_heads[..., half_dim:]
    return jnp.concatenate([front_half * cosine - back_half * sine_table, back_half * cosine + front_half * sine_table], axis=-1)

def attend(queries, key_heads, value_heads, query_pos, key_pos):
    scaling = 1.0 / math.sqrt(queries.shape[-1])
    scores = jnp.einsum('rgad,kgd->grak', queries.astype(jnp.float32), key_heads) * scaling
    if query_pos is not None:
        allowed = key_pos[None, None, None, :] <= query_pos[None, :, None, None]
        scores = jnp.where(allowed, scores, -jnp.inf)
    running_max = lax.optimization_barrier(jnp.max(scores, axis=-1, keepdims=True))
    weights = jnp.exp(scores - running_max)
    normalizer = lax.optimization_barrier(jnp.sum(weights, axis=-1))
    rounded = lax.optimization_barrier(weights.astype(jnp.bfloat16)).astype(jnp.float32)
    weighted = jnp.einsum('grak,kgd->rgad', rounded, value_heads)
    return (weighted / jnp.transpose(normalizer, (1, 0, 2))[..., None]).astype(jnp.bfloat16)

def reference(hidden_states, query_states, w_query, w_key, w_value, slot_order):
    sharing = HEADS // KV_HEADS
    row_ids = jnp.arange(SEQ, dtype=jnp.int32)
    positions = (slot_order[row_ids // SPAN] * SPAN + row_ids % SPAN).astype(jnp.int32)
    pos_float = positions.astype(jnp.float32)
    query_sum = jnp.dot(hidden_states, w_query, preferred_element_type=jnp.float32)
    queries = rotate(query_sum.reshape(SEQ, HEADS, HEAD_DIM), pos_float).astype(jnp.bfloat16)
    key_sum = jnp.dot(hidden_states, w_key, preferred_element_type=jnp.float32)
    key_heads = rotate(key_sum.reshape(SEQ, KV_HEADS, HEAD_DIM), pos_float).astype(jnp.bfloat16)
    value_heads = jnp.dot(hidden_states, w_value, preferred_element_type=jnp.float32).astype(jnp.bfloat16)
    keys_wide = key_heads.astype(jnp.float32)
    values_wide = value_heads.reshape(SEQ, KV_HEADS, HEAD_DIM).astype(jnp.float32)
    block_size = math.gcd(SEQ, 128)
    grouped = queries.reshape(SEQ // block_size, block_size, KV_HEADS, sharing, HEAD_DIM)
    spans = positions.reshape(SEQ // block_size, block_size)

    def one_block(paired):
        return attend(paired[0], keys_wide, values_wide, paired[1], positions)
    attention = lax.map(one_block, (grouped, spans)).reshape(SEQ, HEADS * HEAD_DIM)
    fresh_pos = jnp.full((QUERIES,), SEQ, jnp.float32)
    decode_sum = jnp.dot(query_states, w_query, preferred_element_type=jnp.float32)
    decode_query = rotate(decode_sum.reshape(QUERIES, HEADS, HEAD_DIM), fresh_pos).astype(jnp.bfloat16)
    decode_query = decode_query.reshape(QUERIES, KV_HEADS, sharing, HEAD_DIM)
    decoded = attend(decode_query, keys_wide, values_wide, None, None).reshape(QUERIES, HEADS * HEAD_DIM)
    return (attention, decoded)
```

```python
import math

import jax
import jax.numpy as jnp
from jax import lax
from jax.experimental import pallas as pl
from jax.experimental.pallas import tpu as pltpu
from jax.sharding import Mesh
from jax.sharding import PartitionSpec as P

HEAD_DIM = 128
ROPE_BASE = 500000.0
FLOOR = -1e30
CEILING = 1e30
BLK = ("z", "yl")
BF16 = jnp.bfloat16
F32 = jnp.float32


TILE = 256


def shift(x, axis, by):
    n = lax.axis_size(axis)
    return lax.ppermute(x, axis, [(i, (i + by) % n) for i in range(n)])


def tables(position):
    frequency = jnp.float32(ROPE_BASE) ** (
        jnp.arange(HEAD_DIM // 2, dtype=F32) * jnp.float32(-2.0 / HEAD_DIM)
    )
    angles = position.astype(F32)[:, None] * frequency[None, :]
    cosine, sine = jnp.cos(angles), jnp.sin(angles)
    return jnp.concatenate([cosine, cosine], 1), jnp.concatenate([-sine, sine], 1)


def rotated(x, cosine, sine):
    return x * cosine + pltpu.roll(x, HEAD_DIM // 2, 1) * sine


def kv_kernel(mine, other, cosine, sine, out):
    rows = mine.shape[0]
    x = mine[...] + other[...]
    out[0] = rotated(x[:, :HEAD_DIM], cosine[...], sine[...]).astype(BF16)
    for t in range(rows // 128):
        piece = x[128 * t : 128 * t + 128, HEAD_DIM:]
        out[1, 128 * t : 128 * t + 128, :] = piece.T.astype(BF16)


def q_kernel(mine, other, cosine, sine, fresh_cosine, fresh_sine, out):
    heads = mine.shape[1] // HEAD_DIM
    rows = cosine.shape[0]
    fresh = fresh_cosine.shape[0]
    asked = []
    for h in range(heads):
        cols = slice(h * HEAD_DIM, (h + 1) * HEAD_DIM)
        x = mine[:rows, cols] + other[:rows, cols]
        out[:, h * rows : (h + 1) * rows] = rotated(x, cosine[...], sine[...]).T.astype(BF16)
        x = mine[rows : rows + fresh, cols] + other[rows : rows + fresh, cols]
        asked.append(rotated(x, fresh_cosine[...], fresh_sine[...]))
    asked.append(jnp.zeros((128 - heads * fresh, HEAD_DIM), F32))
    out[:, heads * rows :] = jnp.concatenate(asked, 0).T.astype(BF16)


def attend_kernel(first, n_arrays, split, *refs):
    meta, info, queries = refs[:3]
    kv = refs[3 : 3 + n_arrays]
    refs = refs[3 + n_arrays :]
    if first:
        state = None
    else:
        state, refs = refs[0], refs[1:]
    out, keys, vals, s0, s1, probs = refs
    chunks = 2 if split else 2 * n_arrays
    rows = keys.shape[0] // chunks
    half = rows // 2
    for chunk in range(chunks):
        n, ab = divmod(chunk, 2)
        k_src = kv[0].at[ab] if split else kv[n].at[0, ab]
        v_src = kv[1].at[ab] if split else kv[n].at[1, ab]
        keys[chunk * rows : (chunk + 1) * rows, :] = k_src[...]
        for t in range(rows // 128):
            at = chunk * rows + 128 * t
            vals[:, at : at + 128] = v_src[128 * t : 128 * t + 128, :]
    granules = 2 * chunks
    tiles = queries.shape[1] // TILE
    scale = math.log2(math.e) / math.sqrt(HEAD_DIM)

    def scores(i, s):
        at = pl.multiple_of(i * TILE, TILE)
        s[...] = jnp.dot(keys[...], queries[:, pl.ds(at, TILE)], preferred_element_type=F32)

    def update(i, s):
        at = pl.multiple_of(i * TILE, TILE)
        q_pos = info[0:1, pl.ds(at, TILE)]
        q_seg = info[1:2, pl.ds(at, TILE)]
        top = jnp.full((1, TILE), FLOOR, F32) if first else state[128:129, pl.ds(at, TILE)]
        best = top
        allow = []
        for g in range(granules):
            at_g = slice(g * half, (g + 1) * half)
            block = s[at_g, :]
            if first and g < 2:
                ids = lax.broadcasted_iota(jnp.int32, (half, TILE), 0)
                block = jnp.where(ids <= q_pos - meta[granules + g], block, FLOOR)
                s[at_g, :] = block
                allow.append(None)
                best = jnp.maximum(best, jnp.max(block, axis=0, keepdims=True))
            else:
                ok = q_seg > meta[g]
                allow.append(ok)
                high = jnp.max(block, axis=0, keepdims=True)
                best = jnp.maximum(best, jnp.where(ok, high, FLOOR))
        total = jnp.zeros((1, TILE), F32)
        for g in range(granules):
            at_g = slice(g * half, (g + 1) * half)
            base = best if allow[g] is None else jnp.where(allow[g], best, CEILING)
            p = jnp.exp2((s[at_g, :] - base) * scale)
            total = total + jnp.sum(p, axis=0, keepdims=True)
            probs[at_g, :] = p.astype(BF16)
        new = jnp.dot(vals[...], probs[...], preferred_element_type=F32)
        if first:
            out[0:128, pl.ds(at, TILE)] = new
        else:
            keep = jnp.exp2((top - best) * scale)
            out[0:128, pl.ds(at, TILE)] = state[0:128, pl.ds(at, TILE)] * keep + new
            total = total + state[136:137, pl.ds(at, TILE)] * keep
        out[128:136, pl.ds(at, TILE)] = jnp.broadcast_to(best, (8, TILE))
        out[136:144, pl.ds(at, TILE)] = jnp.broadcast_to(total, (8, TILE))

    scores(0, s0)

    def pair(j, _):
        i = 2 * j
        scores(i + 1, s1)
        update(i, s0)
        scores(i + 2, s0)
        update(i + 1, s1)
        return 0

    lax.fori_loop(0, (tiles - 1) // 2, pair, 0)
    if tiles % 2 == 0:
        scores(tiles - 1, s1)
        update(tiles - 2, s0)
        update(tiles - 1, s1)
    else:
        update(tiles - 1, s0)


def attend(meta, info, queries, arrays, state, split=False):
    rows = arrays[0].shape[-2]
    chunks = 2 if split else 2 * len(arrays)
    columns = queries.shape[1]
    count = chunks * rows
    smem = pl.BlockSpec(memory_space=pltpu.SMEM)
    vmem = pl.BlockSpec(memory_space=pltpu.VMEM)
    first = state is None
    operands = [meta, info, queries, *arrays] + ([] if first else [state])

    def kernel(*refs):
        attend_kernel(first, len(arrays), split, *refs)

    return pl.pallas_call(
        kernel,
        in_specs=[smem] + [vmem] * (len(operands) - 1),
        out_specs=vmem,
        out_shape=jax.ShapeDtypeStruct((144, columns), F32),
        scratch_shapes=[
            pltpu.VMEM((count, HEAD_DIM), BF16),
            pltpu.VMEM((HEAD_DIM, count), BF16),
            pltpu.VMEM((count, TILE), F32),
            pltpu.VMEM((count, TILE), F32),
            pltpu.VMEM((count, TILE), BF16),
        ],
        cost_estimate=pl.CostEstimate(
            flops=4 * count * columns * HEAD_DIM,
            transcendentals=count * columns,
            bytes_accessed=2 * 144 * columns * 4 + columns * 256 + count * 512,
        ),
        name="attend",
    )(*operands)


def merge_kernel(fresh, mine, other, out):
    scale = math.log2(math.e) / math.sqrt(HEAD_DIM)
    part = mine.shape[1]
    doc = part - 128
    rows = doc // 4
    half = rows // 2
    top_a, top_b = mine[128:129, :], other[128:129, :]
    best = jnp.maximum(top_a, top_b)
    by_a, by_b = jnp.exp2((top_a - best) * scale), jnp.exp2((top_b - best) * scale)
    total = mine[136:137, :] * by_a + other[136:137, :] * by_b
    result = (mine[0:128, :] * by_a + other[0:128, :] * by_b) / total
    asked = result[:, doc:].T
    for h in range(4):
        cols = slice(h * HEAD_DIM, (h + 1) * HEAD_DIM)
        turned = result[:, h * rows : (h + 1) * rows].T.astype(BF16)
        for j in range(2):
            out[j, :half, cols] = turned[j * half : (j + 1) * half]
    pad = jnp.zeros((16 - fresh // 2, 4 * HEAD_DIM), F32)
    for j in range(2):
        each = [asked[h * fresh + j * (fresh // 2) : h * fresh + (j + 1) * (fresh // 2)] for h in range(4)]
        out[j, half:, :] = jnp.concatenate([jnp.concatenate(each, 1), pad], 0).astype(BF16)


def call(kernel, shape, *operands):
    vmem = pl.BlockSpec(memory_space=pltpu.VMEM)
    return pl.pallas_call(
        kernel,
        in_specs=[vmem] * len(operands),
        out_specs=vmem,
        out_shape=shape,
    )(*operands)


def body(hidden, asking, w_query, w_key, w_value, slot_order):
    zs, yls = lax.axis_size("z"), lax.axis_size("yl")
    z, yl, tp = lax.axis_index("z"), lax.axis_index("yl"), lax.axis_index("tp")
    yh, co = lax.axis_index("yh"), lax.axis_index("co")
    blk = z * yls + yl
    half, width = hidden.shape
    rows = 2 * half
    span = 2 * half
    seq = 4 * half * zs * yls
    each = asking.shape[0] // (zs * yls)
    fresh = 2 * each

    own = jnp.concatenate(
        [
            hidden,
            lax.dynamic_slice_in_dim(asking, each * blk, each, 0),
            jnp.zeros((16 - each, width), BF16),
        ],
        0,
    )
    cut = own.shape[0] // 2
    from_low = shift(own, "tp", 1)
    from_high = shift(own, "tp", -1)
    far_a = shift(from_low[:cut], "tp", 1)
    far_b = shift(from_high[cut:], "tp", -1)
    pieces = jnp.stack([own, from_high, jnp.concatenate([far_a, far_b], 0), from_low])

    def piece(p):
        return lax.dynamic_index_in_dim(pieces, (p - tp) % 4, 0, keepdims=False)

    mine_0, mine_1 = piece(co), piece(co + 2)
    peer_0, peer_1 = piece(1 - co), piece(3 - co)
    mine_rows = jnp.concatenate([mine_0[:half], mine_1[:half]], 0)
    peer_rows = jnp.concatenate([peer_0[:half], peer_1[:half]], 0)

    def with_asking(doc, a, b):
        pad = jnp.zeros((16 - fresh, width), BF16)
        return jnp.concatenate([doc, a[half : half + each], b[half : half + each], pad], 0)

    def cols(w, which, size):
        return lax.dynamic_slice_in_dim(w, which * size, size, 1)

    w_kv = jnp.concatenate(
        [
            cols(w_key, yh, HEAD_DIM),
            cols(w_value, yh, HEAD_DIM),
            cols(w_key, 1 - yh, HEAD_DIM),
            cols(w_value, 1 - yh, HEAD_DIM),
        ],
        1,
    )
    q_cols = w_query.shape[1] // 2
    w_q = jnp.concatenate([cols(w_query, yh, q_cols), cols(w_query, 1 - yh, q_cols)], 1)

    order = slot_order
    seg = lax.dynamic_slice_in_dim(order, 2 * blk, 2, 0)
    inside = jnp.arange(half, dtype=jnp.int32)

    def row_positions(c):
        return jnp.concatenate([seg[j] * span + half * c + inside for j in range(2)])

    own_pos, peer_pos = row_positions(co), row_positions(1 - co)
    cosine, sine = tables(own_pos)
    fresh_cosine, fresh_sine = tables(jnp.full((fresh,), seq, jnp.int32))
    late = jnp.full((128,), seq, jnp.int32)
    late_seg = jnp.full((128,), order.shape[0], jnp.int32)
    q_seg = jnp.repeat(seg, half)
    q_seg = jnp.concatenate([q_seg, q_seg, q_seg, q_seg, late_seg])
    q_pos = jnp.concatenate(
        [own_pos, own_pos, own_pos, own_pos, late, peer_pos, peer_pos, peer_pos, peer_pos, late]
    )
    info = jnp.stack([q_pos, jnp.concatenate([q_seg, q_seg])] + [jnp.zeros_like(q_pos)] * 6)

    def segments(z_of):
        first = 2 * ((z_of % zs) * yls + yl)
        second = 2 * ((z_of % zs) * yls + (1 - yl))
        return jnp.concatenate(
            [lax.dynamic_slice_in_dim(order, first, 2, 0), lax.dynamic_slice_in_dim(order, second, 2, 0)]
        )

    far = shift(jnp.dot(peer_rows, w_kv, preferred_element_type=F32), "co", 1)
    kv_sum = jnp.dot(mine_rows, w_kv, preferred_element_type=F32) + far
    kv_far = shift(kv_sum[:, 2 * HEAD_DIM :], "yh", 1)
    kv = call(
        kv_kernel,
        jax.ShapeDtypeStruct((2, rows, HEAD_DIM), BF16),
        kv_sum[:, : 2 * HEAD_DIM],
        kv_far,
        cosine,
        sine,
    )
    unit = jnp.stack([kv, shift(kv, "yl", 1)], 1)

    q_peer = jnp.dot(with_asking(peer_rows, peer_0, peer_1), w_q, preferred_element_type=F32)
    q_sum = jnp.dot(with_asking(mine_rows, mine_0, mine_1), w_q, preferred_element_type=F32) + shift(
        q_peer, "co", 1
    )
    q_far = shift(q_sum[:, q_cols:], "yh", 1)
    part = 4 * rows + 128
    queries = call(
        q_kernel,
        jax.ShapeDtypeStruct((HEAD_DIM, part), BF16),
        q_sum[:, :q_cols],
        q_far,
        cosine,
        sine,
        fresh_cosine,
        fresh_sine,
    )
    queries = jnp.concatenate([queries, shift(queries, "co", 1)], 1)

    up, down = shift(unit, "z", 1), shift(unit, "z", -1)
    bases = jnp.stack([seg[j] * span + half * co for j in range(2)])
    state = attend(jnp.concatenate([segments(z), bases]), info, queries, [unit], None)
    for step in range(1, zs // 2):
        if step < zs // 2 - 1:
            next_up, next_down = shift(up, "z", 1), shift(down, "z", -1)
        else:
            next_up, next_down = shift(up[0], "z", 1), shift(down[1], "z", -1)
        meta = jnp.concatenate([segments(z - step), segments(z + step)])
        state = attend(meta, info, queries, [up, down], state)
        up, down = next_up, next_down
    state = attend(segments(z + zs // 2), info, queries, [up, down], state, split=True)

    other = shift(state[:, part:], "co", 1)

    def kernel(*refs):
        merge_kernel(fresh, *refs)

    merged = call(
        kernel, jax.ShapeDtypeStruct((2, half + 16, 4 * HEAD_DIM), BF16), state[:, :part], other
    )
    kept = lax.dynamic_index_in_dim(merged, yh, 0, keepdims=False)
    came = shift(lax.dynamic_index_in_dim(merged, 1 - yh, 0, keepdims=False), "yh", 1)
    whole = jnp.where(
        yh == 0, jnp.concatenate([kept, came], 1), jnp.concatenate([came, kept], 1)
    )
    decoded = lax.all_gather(whole[half : half + each], BLK, axis=0, tiled=True)
    return whole[:half], decoded


def solution(mesh):
    n_blk, n_tp, n_qg = (mesh.shape[a] for a in ("blk", "tp", "qg"))
    finer = Mesh(
        mesh.devices.reshape(n_blk // 2, 2, n_tp, n_qg // 2, 2), ("z", "yl", "tp", "yh", "co")
    )
    qg = ("yh", "co")
    return jax.shard_map(
        body,
        mesh=finer,
        in_specs=(P(("z", "yl", "tp"), qg), P("tp", qg), P(qg, "tp"), P(qg, "tp"), P(qg, "tp"), P()),
        out_specs=(P(("z", "yl", "yh", "co"), "tp"), P(qg, "tp")),
        check_vma=False,
    )
```

```python
import math

import jax
import jax.numpy as jnp
from jax import lax
from jax.experimental import pallas as pl
from jax.experimental.pallas import tpu as pltpu
from jax.sharding import Mesh
from jax.sharding import PartitionSpec as P

HEAD_DIM = 128
ROPE_BASE = 500000.0
FLOOR = -1e30
CEILING = 1e30
BLK = ("z", "yl")
BF16 = jnp.bfloat16
F32 = jnp.float32
TILE = 256
SCALE = math.log2(math.e) / math.sqrt(HEAD_DIM)


OUT_TYPE = pltpu.VMEM

SMEM = pl.BlockSpec(memory_space=pltpu.SMEM)
VMEM = pl.BlockSpec(memory_space=pltpu.VMEM)


def shift(x, axis, by):
    n = lax.axis_size(axis)
    return lax.ppermute(x, axis, [(i, (i + by) % n) for i in range(n)])


def tables(position):
    lane = jnp.arange(HEAD_DIM, dtype=jnp.int32)
    frequency = jnp.float32(ROPE_BASE) ** (
        (lane % (HEAD_DIM // 2)).astype(F32) * jnp.float32(-2.0 / HEAD_DIM)
    )
    angles = position.astype(F32) * frequency[None, :]
    return jnp.cos(angles), jnp.where(lane < HEAD_DIM // 2, -1.0, 1.0) * jnp.sin(angles)


def rotated(x, cosine, sine):
    return x * cosine + pltpu.roll(x, HEAD_DIM // 2, 1) * sine


def own_pieces(ids):
    tp, co = ids[2], ids[4]
    group = (tp + co) % 2
    mine, peer = (tp + group) % 4, (tp + 1 - group) % 4
    return (mine, (mine + 2) % 4), (peer, (peer + 2) % 4)


def sided(ids, use):
    group = (ids[2] + ids[4]) % 2
    for g in range(2):
        pl.when(group == g)(lambda g=g: use(g))


def kv_project_kernel(ids, own, high, low, far_a, far_b, w_k, w_v, near, far, peer, w):
    yh = ids[3]
    for i, side in enumerate((yh, 1 - yh)):
        cols = pl.ds(pl.multiple_of(side * HEAD_DIM, HEAD_DIM), HEAD_DIM)
        w[:, 2 * i * HEAD_DIM : (2 * i + 1) * HEAD_DIM] = w_k[:, cols]
        w[:, (2 * i + 1) * HEAD_DIM : (2 * i + 2) * HEAD_DIM] = w_v[:, cols]
    groups = ((own, far_a, far_b), (high, low))

    def use(g):
        for mine in (False, True):
            at = 0
            for x in groups[g if mine else 1 - g]:
                there = slice(at, at + x.shape[0])
                at += x.shape[0]
                y = jnp.dot(x[...], w[...], preferred_element_type=F32)
                if mine:
                    near[there, :] = y[:, : 2 * HEAD_DIM]
                    far[there, :] = y[:, 2 * HEAD_DIM :]
                else:
                    peer[there, :] = y

    sided(ids, use)


def q_project_kernel(each, ids, own, high, low, far_a, far_b, *refs):
    asked, (w, near, far, peer) = refs[:4], refs[4:]
    yh = ids[3]
    rows = 2 * own.shape[0]
    width = near.shape[1]
    groups = ((own, far_a, far_b), (high, low))
    fresh = ((asked[0], asked[3]), (asked[1], asked[2]))
    sides = [
        pl.ds(pl.multiple_of(side * width, width), width) for side in (yh, 1 - yh)
    ]

    def use(g):
        for mine in (False, True):
            k = g if mine else 1 - g
            outs = (near, far) if mine else (peer.at[:, :width], peer.at[:, width:])
            for cols, out in zip(sides, outs):
                at = 0
                for x in groups[k]:
                    there = slice(at, at + x.shape[0])
                    at += x.shape[0]
                    out[there, :] = jnp.dot(x[...], w[:, cols], preferred_element_type=F32)
                x = jnp.concatenate([fresh[k][0][...], fresh[k][1][...]], 0)
                x = jnp.dot(x, w[:, cols], preferred_element_type=F32)
                pad = jnp.zeros((16 - 2 * each, width), F32)
                out[rows:, :] = jnp.concatenate([x[:each], x[16 : 16 + each], pad], 0)

    sided(ids, use)


def kv_kernel(mine, arrived, other, cosine, sine, out):
    rows = mine.shape[0]
    x = mine[...] + arrived[:, : mine.shape[1]] + other[...]
    out[0] = rotated(x[:, :HEAD_DIM], cosine[...], sine[...]).astype(BF16)
    for t in range(rows // 128):
        piece = x[128 * t : 128 * t + 128, HEAD_DIM:]
        out[1, 128 * t : 128 * t + 128, :] = piece.T.astype(BF16)


def pair_kernel(a, b, out):
    for i in range(2):
        out[i, 0] = a[i]
        out[i, 1] = b[i]


def q_kernel(mine, arrived, other, cosine, sine, fresh_cosine, fresh_sine, out):
    heads = mine.shape[1] // HEAD_DIM
    rows = cosine.shape[0]
    fresh = fresh_cosine.shape[0]
    asked = []
    for h in range(heads):
        cols = slice(h * HEAD_DIM, (h + 1) * HEAD_DIM)
        x = mine[:rows, cols] + arrived[:rows, cols] + other[:rows, cols]
        out[:, h * rows : (h + 1) * rows] = rotated(x, cosine[...], sine[...]).T.astype(BF16)
        late = slice(rows, rows + fresh)
        x = mine[late, cols] + arrived[late, cols] + other[late, cols]
        asked.append(rotated(x, fresh_cosine[...], fresh_sine[...]))
    asked.append(jnp.zeros((128 - heads * fresh, HEAD_DIM), F32))
    out[:, heads * rows :] = jnp.concatenate(asked, 0).T.astype(BF16)


def attend_kernel(first, n_arrays, split, origins, shape, tile_0, *refs):
    ids, order, queries = refs[:3]
    kv = refs[3 : 3 + n_arrays]
    refs = refs[3 + n_arrays :]
    if first:
        state = None
    else:
        state, refs = refs[0], refs[1:]
    out, keys, vals, s0, s1, m0, m1, probs = refs
    chunks = 2 if split else 2 * n_arrays
    rows = keys.shape[0] // chunks
    half = rows // 2
    for chunk in range(chunks):
        n, ab = divmod(chunk, 2)
        k_src = kv[0].at[ab] if split else kv[n].at[0, ab]
        v_src = kv[1].at[ab] if split else kv[n].at[1, ab]
        keys[chunk * rows : (chunk + 1) * rows, :] = k_src[...]
        for t in range(rows // 128):
            at = chunk * rows + 128 * t
            vals[:, at : at + 128] = v_src[128 * t : 128 * t + 128, :]
    granules = 2 * chunks
    tiles = out.shape[1] // TILE
    zs, yls, doc_tiles = shape
    span = 4 * half
    mine, peer = own_pieces(ids)
    own_seg, peer_seg = [
        [order[2 * (ids[0] * yls + ids[1]) + p // 2] for p in pair] for pair in (mine, peer)
    ]
    own_start = [seg * (span // 2) + (p % 2) * half for seg, p in zip(own_seg, mine)]
    peer_start = [seg * (span // 2) + (p % 2) * half for seg, p in zip(peer_seg, peer)]
    meta = []
    for dz, flip in origins:
        block = (ids[0] + (dz + zs)) % zs * yls + (1 - ids[1] if flip else ids[1])
        meta += [order[2 * block + p // 2] for p in mine]
    lane = lax.broadcasted_iota(jnp.int32, (1, TILE), 1)

    def columns(i):
        t = i + tile_0
        r = lane + (t * TILE) % (2 * half)
        r = jnp.where(r >= 2 * half, r - 2 * half, r)
        second = r >= half
        late, others = t >= 2 * doc_tiles, t >= doc_tiles
        seg = [jnp.where(late, 1 << 20, jnp.where(others, b, a)) for a, b in zip(own_seg, peer_seg)]
        start = [
            jnp.where(late, 1 << 29, jnp.where(others, b, a)) for a, b in zip(own_start, peer_start)
        ]
        return r, second, seg, start

    def place(i, base=0):
        i = i + base
        return pl.ds(i * TILE if isinstance(i, int) else pl.multiple_of(i * TILE, TILE), TILE)

    def scores(i, s, m, chunk):
        block = jnp.dot(
            keys[chunk * rows : (chunk + 1) * rows, :],
            queries[:, place(i, tile_0)],
            preferred_element_type=F32,
        )
        for j in range(2):
            g = 2 * chunk + j
            part = block[j * half : (j + 1) * half]
            if first and g < 2:
                row = lax.broadcasted_iota(jnp.int32, (half, TILE), 0)
                r, second, _, start = columns(i)
                q_pos = r + jnp.where(second, start[1] - half, start[0])
                part = jnp.where(row <= q_pos - own_start[g], part, FLOOR)
            s[g * half : (g + 1) * half, :] = part
            m[g : g + 1, :] = jnp.max(part, axis=0, keepdims=True)

    def begin(i, m):
        _, second, seg, _ = columns(i)
        q_seg = jnp.where(second, seg[1], seg[0])
        top = jnp.full((1, TILE), FLOOR, F32) if first else state[128:129, place(i, tile_0)]
        best = top
        allow = []
        for g in range(granules):
            high = m[g : g + 1, :]
            if first and g < 2:
                allow.append(None)
                best = jnp.maximum(best, high)
            else:
                ok = q_seg > meta[g]
                allow.append(ok)
                best = jnp.maximum(best, jnp.where(ok, high, FLOOR))
        bases = [best if ok is None else jnp.where(ok, best, CEILING) for ok in allow]
        return top, best, bases

    def weigh(s, bases, chunk, total):
        for g in (2 * chunk, 2 * chunk + 1):
            at_g = slice(g * half, (g + 1) * half)
            p = jnp.exp2((s[at_g, :] - bases[g]) * SCALE)
            total = total + jnp.sum(p, axis=0, keepdims=True)
            probs[at_g, :] = p.astype(BF16)
        return total

    def product(chunk):
        at_c = slice((chunk - 1) * rows, (chunk + 1) * rows)
        return jnp.dot(vals[:, at_c], probs[at_c, :], preferred_element_type=F32)

    def finish(i, top, best, total, new):
        if not first:
            keep = jnp.exp2((top - best) * SCALE)
            new = state[0:128, place(i, tile_0)] * keep + new
            total = total + state[136:137, place(i, tile_0)] * keep
        out[0:128, place(i)] = new
        out[128:136, place(i)] = jnp.broadcast_to(best, (8, TILE))
        out[136:144, place(i)] = jnp.broadcast_to(total, (8, TILE))

    def step(i, s, m, ahead=None):
        top, best, bases = begin(i, m)
        total = jnp.zeros((1, TILE), F32)
        new = None
        for chunk in range(chunks):
            if ahead is not None:
                scores(*ahead, chunk)
            total = weigh(s, bases, chunk, total)
            if chunk % 2:
                more = product(chunk)
                new = more if new is None else new + more
        finish(i, top, best, total, new)

    for chunk in range(chunks):
        scores(0, s0, m0, chunk)
    if tiles > 1:

        def pair(j, _):
            i = 2 * j
            step(i, s0, m0, (i + 1, s1, m1))
            step(i + 1, s1, m1, (i + 2, s0, m0))
            return 0

        lax.fori_loop(0, (tiles - 1) // 2, pair, 0)
    if tiles % 2 == 0:
        step(tiles - 2, s0, m0, (tiles - 1, s1, m1))
        step(tiles - 1, s1, m1)
    else:
        step(tiles - 1, s0, m0)


def held(x):
    return pltpu.with_memory_space_constraint(x, pltpu.VMEM)


def attend(ids, order, queries, arrays, state, origins, shape, split=False, lanes=None):
    rows = arrays[0].shape[-2]
    chunks = 2 if split else 2 * len(arrays)
    at, columns = lanes or (0, queries.shape[1])
    count = chunks * rows
    first = state is None
    operands = [ids, order] + [held(x) for x in (queries, *arrays, *(() if first else (state,)))]

    def kernel(*refs):
        attend_kernel(first, len(arrays), split, origins, shape, at // TILE, *refs)

    return pl.pallas_call(
        kernel,
        in_specs=[SMEM, SMEM] + [VMEM] * (len(operands) - 2),
        out_specs=VMEM,
        out_shape=OUT_TYPE((144, columns), F32),
        scratch_shapes=[
            pltpu.VMEM((count, HEAD_DIM), BF16),
            pltpu.VMEM((HEAD_DIM, count), BF16),
            pltpu.VMEM((count, TILE), F32),
            pltpu.VMEM((count, TILE), F32),
            pltpu.VMEM((8, TILE), F32),
            pltpu.VMEM((8, TILE), F32),
            pltpu.VMEM((count, TILE), BF16),
        ],
        cost_estimate=pl.CostEstimate(
            flops=4 * count * columns * HEAD_DIM,
            transcendentals=count * columns,
            bytes_accessed=2 * 144 * columns * 4 + columns * 256 + count * 512,
        ),
        compiler_params=pltpu.CompilerParams(vmem_limit_bytes=20 << 20),
        name="attend",
    )(*operands)


def merged(mine, other):
    mine = mine.at[:, : other.shape[1]]
    top_a, top_b = mine[128:129, :], other[128:129, :]
    best = jnp.maximum(top_a, top_b)
    by_a, by_b = jnp.exp2((top_a - best) * SCALE), jnp.exp2((top_b - best) * SCALE)
    total = mine[136:137, :] * by_a + other[136:137, :] * by_b
    return (mine[0:128, :] * by_a + other[0:128, :] * by_b) / total


def merge_kernel(ids, mine, other, kept, sent, both):
    result = merged(mine, other)
    half = kept.shape[0]
    for h in range(4):
        cols = slice(h * HEAD_DIM, (h + 1) * HEAD_DIM)
        turned = result[:, 2 * h * half : 2 * (h + 1) * half].T.astype(BF16)
        for j in range(2):
            both[j, :, cols] = turned[j * half : (j + 1) * half]
    keep = jnp.where(own_pieces(ids)[0][0] // 2 == ids[3], 0, 1)
    kept[...] = both[keep]
    sent[...] = both[1 - keep]


def merge_asked_kernel(ids, mine, other, kept, sent):
    each = 4
    asked = merged(mine, other).T
    pad = jnp.zeros((16 - each, 4 * HEAD_DIM), F32)
    both = []
    for j in range(2):
        rows = [asked[(2 * h + j) * each : (2 * h + j + 1) * each] for h in range(4)]
        both.append(jnp.concatenate([jnp.concatenate(rows, 1), pad], 0).astype(BF16))
    first = own_pieces(ids)[0][0] // 2 == ids[3]
    kept[...] = jnp.where(first, both[0], both[1])
    sent[...] = jnp.where(first, both[1], both[0])


def call(kernel, shape, operands, scalars=0, scratch=(), flops=0, name=None):
    many = isinstance(shape, (list, tuple))
    return pl.pallas_call(
        kernel,
        in_specs=[SMEM] * scalars + [VMEM] * (len(operands) - scalars),
        out_specs=[VMEM] * len(shape) if many else VMEM,
        out_shape=shape,
        scratch_shapes=list(scratch),
        cost_estimate=pl.CostEstimate(flops=flops, transcendentals=0, bytes_accessed=1 << 20),
        compiler_params=pltpu.CompilerParams(vmem_limit_bytes=20 << 20),
        name=name,
    )(*operands[:scalars], *map(held, operands[scalars:]))


def arr(*shape, dtype=F32):
    return OUT_TYPE(shape, dtype)


def body(hidden, asking, w_query, w_key, w_value, slot_order):
    zs, yls = lax.axis_size("z"), lax.axis_size("yl")
    z, yl, tp = lax.axis_index("z"), lax.axis_index("yl"), lax.axis_index("tp")
    yh, co = lax.axis_index("yh"), lax.axis_index("co")
    blk = z * yls + yl
    half, width = hidden.shape
    rows = 2 * half
    span = 2 * half
    seq = 4 * half * zs * yls
    each = asking.shape[0] // (zs * yls)
    fresh = 2 * each

    cut = half // 2
    low = shift(hidden, "tp", 1)
    high = shift(hidden, "tp", -1)
    far_a = shift(low[:cut], "tp", 1)
    far_b = shift(high[cut:], "tp", -1)
    pieces = (hidden, high, low, far_a, far_b)
    own_asks = jnp.pad(lax.dynamic_slice_in_dim(asking, each * blk, each, 0), ((0, 16 - each), (0, 0)))
    asks = (own_asks, shift(own_asks, "tp", -1), shift(own_asks, "tp", 1), shift(own_asks, "tp", 2))

    ids = jnp.stack([z, yl, tp, yh, co]).astype(jnp.int32)
    order = slot_order
    group = (tp + co) % 2
    piece = (tp + group) % 4
    starts = [
        order[2 * blk + p // 2] * span + (p % 2) * half for p in (piece, (piece + 2) % 4)
    ]
    row = jnp.arange(rows, dtype=jnp.int32)[:, None]
    cosine, sine = tables(row + jnp.where(row < half, starts[0], starts[1] - half))
    fresh_cosine, fresh_sine = tables(jnp.full((fresh, 1), seq, jnp.int32))

    kv_near, kv_far, kv_peer = call(
        kv_project_kernel,
        [arr(rows, 2 * HEAD_DIM), arr(rows, 2 * HEAD_DIM), arr(rows, 4 * HEAD_DIM)],
        (ids, *pieces, w_key, w_value),
        1,
        [pltpu.VMEM((width, 4 * HEAD_DIM), BF16)],
        flops=4 * rows * width * 4 * HEAD_DIM,
        name="kv_project",
    )
    arrived = shift(kv_peer, "co", 1)
    kv_other = shift(kv_far + arrived[:, 2 * HEAD_DIM :], "yh", 1)
    kv = call(
        kv_kernel,
        arr(2, rows, HEAD_DIM, dtype=BF16),
        (kv_near, arrived, kv_other, cosine, sine),
        name="kv_rope",
    )
    unit = call(pair_kernel, arr(2, 2, rows, HEAD_DIM, dtype=BF16), (kv, shift(kv, "yl", 1)), name="pair")

    q_cols = w_query.shape[1] // 2

    def q_kernel_of(*refs):
        q_project_kernel(each, *refs)

    asks = lax.optimization_barrier((*asks, kv_peer))[:4]
    q_near, q_far, q_peer = call(
        q_kernel_of,
        [arr(rows + 16, q_cols), arr(rows + 16, q_cols), arr(rows + 16, 2 * q_cols)],
        (ids, *pieces, *asks, w_query),
        1,
        flops=4 * rows * width * 2 * q_cols,
        name="q_project",
    )
    arrived = shift(q_peer, "co", 1)
    q_sent = q_far + arrived[:, q_cols:]
    q_sent, _ = lax.optimization_barrier((q_sent, kv_other))
    other = shift(q_sent, "yh", 1)
    other, unit = lax.optimization_barrier((other, unit))
    doc = 4 * rows
    queries = call(
        q_kernel,
        arr(HEAD_DIM, doc + 128, dtype=BF16),
        (q_near, arrived, other, cosine, sine, fresh_cosine, fresh_sine),
        name="q_rope",
    )
    from_peer = shift(queries, "co", 1)
    queries = jnp.concatenate(
        [queries[:, :doc], from_peer[:, :doc], queries[:, doc:], from_peer[:, doc:]], 1
    )

    def attended(arrays, state, origins, split=False, lanes=None):
        return attend(ids, order, queries, arrays, state, origins, (zs, yls, doc // TILE), split, lanes)

    def origin(*steps):
        return [(dz, flip) for dz in steps for flip in range(2)]

    n = zs // 2
    ups, downs = [unit], [unit]
    state = None
    for step in range(1, n + 1):
        up, down = ups[-1], downs[-1]
        if step > 2:
            done = step - 3
            arrays = [unit] if done == 0 else [ups[done], downs[done]]
            state = attended(arrays, state, origin(*((0,) if done == 0 else (-done, done))))
            state, up, down = lax.optimization_barrier((state, up, down))
        if step == n:
            up, down = up[0], down[1]
        ups.append(shift(up, "z", 1))
        downs.append(shift(down, "z", -1))
    for done in range(n - 2, n):
        state = attended([ups[done], downs[done]], state, origin(-done, done))
    last, last_origin = [ups[n], downs[n]], origin(n)

    asked = attended(last, state, last_origin, True, (2 * doc, 256))
    asked_other = shift(asked[:, 128:], "co", 1)
    theirs = attended(last, state, last_origin, True, (doc, doc))
    doc_other = shift(theirs, "co", 1)
    kept, sent = call(
        merge_asked_kernel,
        [arr(16, 4 * HEAD_DIM, dtype=BF16)] * 2,
        (ids, asked, asked_other),
        1,
        name="merge_asked",
    )

    def whole(kept, sent):
        came = shift(sent, "yh", 1)
        return jnp.where(
            yh == 0, jnp.concatenate([kept, came], 1), jnp.concatenate([came, kept], 1)
        )

    answer = whole(kept, sent)[:each]
    decoded = lax.all_to_all(
        jnp.broadcast_to(answer[None], (zs * yls, *answer.shape)), BLK, 0, 0, tiled=True
    ).reshape(zs * yls * each, -1)
    ours = attended(last, state, last_origin, True, (0, doc))
    kept, sent = call(
        merge_kernel,
        [arr(half, 4 * HEAD_DIM, dtype=BF16)] * 2,
        (ids, ours, doc_other),
        1,
        [pltpu.VMEM((2, half, 4 * HEAD_DIM), BF16)],
        name="merge",
    )
    return whole(kept, sent), decoded


def solution(mesh):
    n_blk, n_tp, n_qg = (mesh.shape[a] for a in ("blk", "tp", "qg"))
    finer = Mesh(
        mesh.devices.reshape(n_blk // 2, 2, n_tp, n_qg // 2, 2), ("z", "yl", "tp", "yh", "co")
    )
    qg = ("yh", "co")
    return jax.shard_map(
        body,
        mesh=finer,
        in_specs=(P(("z", "yl", "tp"), qg), P("tp", qg), P(qg, "tp"), P(qg, "tp"), P(qg, "tp"), P()),
        out_specs=(P(("z", "yl", "yh", "co"), "tp"), P(qg, "tp")),
        check_vma=False,
    )
```

```python
import math

import jax
import jax.numpy as jnp
from jax import lax
from jax.experimental import pallas as pl
from jax.experimental.pallas import tpu as pltpu
from jax.sharding import Mesh
from jax.sharding import PartitionSpec as P

HEAD_DIM = 128
ROPE_BASE = 500000.0
FLOOR = -1e30
CEILING = 1e30
BLK = ("z", "yl")
BF16 = jnp.bfloat16
F32 = jnp.float32
TILE = 256
SCALE = math.log2(math.e) / math.sqrt(HEAD_DIM)


OUT_TYPE = pltpu.VMEM

SMEM = pl.BlockSpec(memory_space=pltpu.SMEM)
VMEM = pl.BlockSpec(memory_space=pltpu.VMEM)


def shift(x, axis, by):
    n = lax.axis_size(axis)
    return lax.ppermute(x, axis, [(i, (i + by) % n) for i in range(n)])


def tables(position):
    lane = jnp.arange(HEAD_DIM, dtype=jnp.int32)
    frequency = jnp.float32(ROPE_BASE) ** (
        (lane % (HEAD_DIM // 2)).astype(F32) * jnp.float32(-2.0 / HEAD_DIM)
    )
    angles = position.astype(F32) * frequency[None, :]
    return jnp.cos(angles), jnp.where(lane < HEAD_DIM // 2, -1.0, 1.0) * jnp.sin(angles)


def rotated(x, cosine, sine):
    return x * cosine + pltpu.roll(x, HEAD_DIM // 2, 1) * sine


def aligned(i, size):
    return pl.ds(pl.multiple_of(i * size, size), size)


def project_kernel(n_pieces, n_asks, joint, ids, *refs):
    pieces, asks = refs[:n_pieces], refs[n_pieces : n_pieces + n_asks]
    w_q, w_k, w_v, *outs = refs[n_pieces + n_asks :]
    w_kv = outs.pop()
    yh, co = ids[3], ids[4]
    q_cols = w_q.shape[1] // 2
    for i, side in enumerate((yh, 1 - yh)):
        at = 2 * i * HEAD_DIM
        w_kv[:, at : at + HEAD_DIM] = w_k[:, aligned(side, HEAD_DIM)]
        w_kv[:, at + HEAD_DIM : at + 2 * HEAD_DIM] = w_v[:, aligned(side, HEAD_DIM)]
    q_sides = [w_q[:, aligned(side, q_cols)] for side in (yh, 1 - yh)]
    kv_sides = [w_kv[:, : 2 * HEAD_DIM], w_kv[:, 2 * HEAD_DIM :]]
    if joint:
        near, far, peer = outs
        each = near.shape[1]
        q_outs = (near.at[:, :q_cols], far.at[:, :q_cols]), (peer.at[:, :q_cols], peer.at[:, each : each + q_cols])
        kv_outs = (near.at[:, q_cols:], far.at[:, q_cols:]), (
            peer.at[:, q_cols:each],
            peer.at[:, each + q_cols :],
        )
    else:
        kv_near, kv_far, kv_peer, near, far, peer = outs
        q_outs = (near, far), (peer.at[:, :q_cols], peer.at[:, q_cols:])
        kv_outs = (kv_near, kv_far), (kv_peer.at[:, : 2 * HEAD_DIM], kv_peer.at[:, 2 * HEAD_DIM :])

    def rows_of(core):
        if n_asks:
            return jnp.where(core == 0, pieces[0][...], pieces[1][...])
        size = pieces[0].shape[0] // 2
        return jnp.concatenate([x[aligned(core, size), :] for x in pieces], 0)

    for group, core in enumerate((co, 1 - co)):
        x = rows_of(core)
        for side in range(2):
            out = kv_outs[group][side]
            out[...] = jnp.dot(x, kv_sides[side], preferred_element_type=F32)
        if n_asks:
            x = jnp.concatenate([x, *[r[...] for r in asks]], 0)
        for side in range(2):
            y = jnp.dot(x, q_sides[side], preferred_element_type=F32)
            out = q_outs[group][side]
            if n_asks:
                at = x.shape[0] - 16 * n_asks
                each_ask = 16 // n_asks
                y = jnp.concatenate(
                    [y[:at]] + [y[at + 16 * i : at + 16 * i + each_ask] for i in range(n_asks)], 0
                )
            out[...] = y


def kv_kernel(ids, *refs):
    phases = [refs[3 * i : 3 * i + 3] for i in range(3)]
    cosine, sine, out, vals = refs[9:]
    at_piece = ([ids[2]], [(ids[2] + 1) % 4, (ids[2] + 3) % 4], [(ids[2] + 2) % 4])
    each = 2 * HEAD_DIM
    for (near, arrived, other), where in zip(phases, at_piece):
        size = near.shape[0] // len(where)
        first = near.shape[1] - each
        for i, p in enumerate(where):
            r = slice(i * size, (i + 1) * size)
            x = near[r, first:] + arrived[r, first : first + each] + other[r, first:]
            there = aligned(p, size)
            turned = rotated(x[:, :HEAD_DIM], cosine[there, :], sine[there, :])
            out[0, there, :] = turned.astype(BF16)
            vals[there, :] = x[:, HEAD_DIM:]
    for t in range(vals.shape[0] // 128):
        out[1, 128 * t : 128 * t + 128, :] = vals[128 * t : 128 * t + 128, :].T.astype(BF16)


def pair_kernel(a, b, out):
    for i in range(2):
        out[i, 0] = a[i]
        out[i, 1] = b[i]


def q_kernel(ids, *refs):
    phases = [refs[3 * i : 3 * i + 3] for i in range(3)]
    cosine, sine, fresh_cosine, fresh_sine, out, late = refs[9:]
    at_piece = ([ids[2]], [(ids[2] + 1) % 4, (ids[2] + 3) % 4], [(ids[2] + 2) % 4])
    heads = 4
    width = heads * HEAD_DIM
    size = cosine.shape[0] // 4
    for (near, arrived, other), where in zip(phases, at_piece):
        for i, p in enumerate(where):
            r = slice(i * size, (i + 1) * size)
            x = near[r, :width] + arrived[r, :width] + other[r, :width]
            there = aligned(p, size)
            turned = [
                rotated(x[:, h * HEAD_DIM : (h + 1) * HEAD_DIM], cosine[there, :], sine[there, :])
                for h in range(heads)
            ]
            out[:, aligned(p, heads * size)] = jnp.concatenate(turned, 0).T.astype(BF16)
    near, arrived, other = phases[2]
    r = slice(size, size + 16)
    x = near[r, :width] + arrived[r, :width] + other[r, :width]
    owners = [ids[2], (ids[2] + 1) % 4, (ids[2] + 3) % 4, (ids[2] + 2) % 4]

    def of_piece(p):
        y = jnp.zeros((4, width), F32)
        for i, owner in enumerate(owners):
            y = y + jnp.where(owner == p, x[4 * i : 4 * i + 4], 0.0)
        return y

    tiles = []
    for core in (ids[4], 1 - ids[4]):
        rows = []
        for k in range(2):
            y = of_piece(core + 2 * k)
            for h in range(heads):
                rows.append(y[:, h * HEAD_DIM : (h + 1) * HEAD_DIM])
        rows = rotated(jnp.concatenate(rows, 0), fresh_cosine[...], fresh_sine[...])
        tiles += [rows, jnp.zeros((128 - rows.shape[0], HEAD_DIM), F32)]
    late[...] = jnp.concatenate(tiles, 0).T.astype(BF16)


def q_pair_kernel(ids, own, came, late, out):
    size = own.shape[1] // 4

    def use(core):
        for side in range(2):
            for k in range(2):
                for part in range(2):
                    p = (core if side == 0 else 1 - core) + 2 * k
                    at = (4 * side + 2 * k + part) * size
                    src = own if part == core else came
                    out[:, at : at + size] = src[:, p * size : (p + 1) * size]

    for core in range(2):
        pl.when(ids[4] == core)(lambda core=core: use(core))
    out[:, 8 * size :] = late[...]


def attend_kernel(first, n_arrays, split, origins, shape, tile_0, *refs):
    ids, order, queries = refs[:3]
    kv = refs[3 : 3 + n_arrays]
    refs = refs[3 + n_arrays :]
    if first:
        state = None
    else:
        state, refs = refs[0], refs[1:]
    out, keys, vals, s0, s1, m0, m1, probs = refs
    chunks = 2 if split else 2 * n_arrays
    rows = keys.shape[0] // chunks
    half = rows // 2
    for chunk in range(chunks):
        n, ab = divmod(chunk, 2)
        k_src = kv[0].at[ab] if split else kv[n].at[0, ab]
        v_src = kv[1].at[ab] if split else kv[n].at[1, ab]
        keys[chunk * rows : (chunk + 1) * rows, :] = k_src[...]
        for t in range(rows // 128):
            at = chunk * rows + 128 * t
            vals[:, at : at + 128] = v_src[128 * t : 128 * t + 128, :]
    granules = 2 * chunks
    tiles = out.shape[1] // TILE
    zs, yls, doc_tiles = shape
    span = 4 * half
    co = ids[4]
    own_seg = [order[2 * (ids[0] * yls + ids[1]) + k] for k in range(2)]
    own_start = [seg * span // 2 + (half // 2) * co for seg in own_seg]
    meta = []
    for dz, flip in origins:
        block = (ids[0] + (dz + zs)) % zs * yls + (1 - ids[1] if flip else ids[1])
        meta += [order[2 * block + k] for k in range(2)]
    lane = lax.broadcasted_iota(jnp.int32, (1, TILE), 1)

    def columns(i):
        t = i + tile_0
        b = t * TILE // (2 * half)
        return lane + (t * TILE - b * (2 * half)), t >= doc_tiles, (b, b + 1)

    def run_seg(b, late):
        return jnp.where(late, 1 << 20, jnp.where(b // 2 % 2 == 0, own_seg[0], own_seg[1]))

    def run_start(b, late):
        seg = jnp.where(b // 2 % 2 == 0, own_seg[0], own_seg[1])
        parity = jnp.where(b < 4, co, 1 - co)
        start = seg * (span // 2) + half * parity + (half // 2) * (b % 2)
        return jnp.where(late, 1 << 29, start)

    def place(i, base=0):
        i = i + base
        return pl.ds(i * TILE if isinstance(i, int) else pl.multiple_of(i * TILE, TILE), TILE)

    def scores(i, s, m, chunk):
        block = jnp.dot(
            keys[chunk * rows : (chunk + 1) * rows, :],
            queries[:, place(i, tile_0)],
            preferred_element_type=F32,
        )
        for j in range(2):
            g = 2 * chunk + j
            part = block[j * half : (j + 1) * half]
            if first and g < 2:
                row = lax.broadcasted_iota(jnp.int32, (half, TILE), 0)
                row = row + jnp.where(row >= half // 2, half // 2, 0)
                r, late, (b0, b1) = columns(i)
                inside = r - (half // 2) * ((r * 683) >> 16)
                q_pos = inside + jnp.where(r >= 2 * half, run_start(b1, late), run_start(b0, late))
                part = jnp.where(row <= q_pos - own_start[g], part, FLOOR)
            s[g * half : (g + 1) * half, :] = part
            m[g : g + 1, :] = jnp.max(part, axis=0, keepdims=True)

    def begin(i, m):
        r, late, (b0, b1) = columns(i)
        q_seg = jnp.where(r >= 2 * half, run_seg(b1, late), run_seg(b0, late))
        top = jnp.full((1, TILE), FLOOR, F32) if first else state[128:129, place(i, tile_0)]
        best = top
        allow = []
        for g in range(granules):
            high = m[g : g + 1, :]
            if first and g < 2:
                allow.append(None)
                best = jnp.maximum(best, high)
            else:
                ok = q_seg > meta[g]
                allow.append(ok)
                best = jnp.maximum(best, jnp.where(ok, high, FLOOR))
        bases = [best if ok is None else jnp.where(ok, best, CEILING) for ok in allow]
        return top, best, bases

    def weigh(s, bases, chunk, total):
        for g in (2 * chunk, 2 * chunk + 1):
            at_g = slice(g * half, (g + 1) * half)
            p = jnp.exp2((s[at_g, :] - bases[g]) * SCALE)
            total = total + jnp.sum(p, axis=0, keepdims=True)
            probs[at_g, :] = p.astype(BF16)
        return total

    def product(chunk):
        at_c = slice((chunk - 1) * rows, (chunk + 1) * rows)
        return jnp.dot(vals[:, at_c], probs[at_c, :], preferred_element_type=F32)

    def finish(i, top, best, total, new):
        if not first:
            keep = jnp.exp2((top - best) * SCALE)
            new = state[0:128, place(i, tile_0)] * keep + new
            total = total + state[136:137, place(i, tile_0)] * keep
        out[0:128, place(i)] = new
        out[128:136, place(i)] = jnp.broadcast_to(best, (8, TILE))
        out[136:144, place(i)] = jnp.broadcast_to(total, (8, TILE))

    def step(i, s, m, ahead=None):
        top, best, bases = begin(i, m)
        total = jnp.zeros((1, TILE), F32)
        new = None
        for chunk in range(chunks):
            if ahead is not None:
                scores(*ahead, chunk)
            total = weigh(s, bases, chunk, total)
            if chunk % 2:
                more = product(chunk)
                new = more if new is None else new + more
        finish(i, top, best, total, new)

    for chunk in range(chunks):
        scores(0, s0, m0, chunk)
    if tiles > 1:

        def pair(j, _):
            i = 2 * j
            step(i, s0, m0, (i + 1, s1, m1))
            step(i + 1, s1, m1, (i + 2, s0, m0))
            return 0

        lax.fori_loop(0, (tiles - 1) // 2, pair, 0)
    if tiles % 2 == 0:
        step(tiles - 2, s0, m0, (tiles - 1, s1, m1))
        step(tiles - 1, s1, m1)
    else:
        step(tiles - 1, s0, m0)


def held(x):
    return pltpu.with_memory_space_constraint(x, pltpu.VMEM)


def attend(ids, order, queries, arrays, state, origins, shape, split=False, lanes=None):
    rows = arrays[0].shape[-2]
    chunks = 2 if split else 2 * len(arrays)
    at, columns = lanes or (0, queries.shape[1])
    count = chunks * rows
    first = state is None
    operands = [ids, order] + [held(x) for x in (queries, *arrays, *(() if first else (state,)))]

    def kernel(*refs):
        attend_kernel(first, len(arrays), split, origins, shape, at // TILE, *refs)

    return pl.pallas_call(
        kernel,
        in_specs=[SMEM, SMEM] + [VMEM] * (len(operands) - 2),
        out_specs=VMEM,
        out_shape=OUT_TYPE((144, columns), F32),
        scratch_shapes=[
            pltpu.VMEM((count, HEAD_DIM), BF16),
            pltpu.VMEM((HEAD_DIM, count), BF16),
            pltpu.VMEM((count, TILE), F32),
            pltpu.VMEM((count, TILE), F32),
            pltpu.VMEM((8, TILE), F32),
            pltpu.VMEM((8, TILE), F32),
            pltpu.VMEM((count, TILE), BF16),
        ],
        cost_estimate=pl.CostEstimate(
            flops=4 * count * columns * HEAD_DIM,
            transcendentals=count * columns,
            bytes_accessed=2 * 144 * columns * 4 + columns * 256 + count * 512,
        ),
        compiler_params=pltpu.CompilerParams(vmem_limit_bytes=20 << 20),
        name="attend",
    )(*operands)


def merged(mine, other):
    mine = mine.at[:, : other.shape[1]]
    top_a, top_b = mine[128:129, :], other[128:129, :]
    best = jnp.maximum(top_a, top_b)
    by_a, by_b = jnp.exp2((top_a - best) * SCALE), jnp.exp2((top_b - best) * SCALE)
    total = mine[136:137, :] * by_a + other[136:137, :] * by_b
    return (mine[0:128, :] * by_a + other[0:128, :] * by_b) / total


def merge_kernel(ids, mine, other, kept, sent, both):
    result = merged(mine, other)
    size = kept.shape[0] // 2
    for k in range(2):
        for part in range(2):
            at = (2 * k + part) * 4 * size
            turned = result[:, at : at + 4 * size].T.astype(BF16)
            for h in range(4):
                cols = slice(h * HEAD_DIM, (h + 1) * HEAD_DIM)
                both[k, part * size : (part + 1) * size, cols] = turned[h * size : (h + 1) * size]
    kept[...] = both[ids[3]]
    sent[...] = both[1 - ids[3]]


def merge_asked_kernel(ids, mine, other, kept, sent):
    each = 4
    asked = merged(mine, other).T
    pad = jnp.zeros((16 - each, 4 * HEAD_DIM), F32)
    both = []
    for k in range(2):
        rows = [asked[(4 * k + h) * each : (4 * k + h + 1) * each] for h in range(4)]
        both.append(jnp.concatenate([jnp.concatenate(rows, 1), pad], 0).astype(BF16))
    first = ids[3] == 0
    kept[...] = jnp.where(first, both[0], both[1])
    sent[...] = jnp.where(first, both[1], both[0])


def call(kernel, shape, operands, scalars=0, scratch=(), flops=0, name=None):
    many = isinstance(shape, (list, tuple))
    return pl.pallas_call(
        kernel,
        in_specs=[SMEM] * scalars + [VMEM] * (len(operands) - scalars),
        out_specs=[VMEM] * len(shape) if many else VMEM,
        out_shape=shape,
        scratch_shapes=list(scratch),
        cost_estimate=pl.CostEstimate(flops=flops, transcendentals=0, bytes_accessed=1 << 20),
        compiler_params=pltpu.CompilerParams(vmem_limit_bytes=20 << 20),
        name=name,
    )(*operands[:scalars], *map(held, operands[scalars:]))


def arr(*shape, dtype=F32):
    return OUT_TYPE(shape, dtype)


def body(hidden, asking, w_query, w_key, w_value, slot_order):
    zs, yls = lax.axis_size("z"), lax.axis_size("yl")
    z, yl, tp = lax.axis_index("z"), lax.axis_index("yl"), lax.axis_index("tp")
    yh, co = lax.axis_index("yh"), lax.axis_index("co")
    blk = z * yls + yl
    half, width = hidden.shape
    rows = 2 * half
    span = 2 * half
    seq = 4 * half * zs * yls
    each = asking.shape[0] // (zs * yls)

    ids = jnp.stack([z, yl, tp, yh, co]).astype(jnp.int32)
    order = slot_order
    row = jnp.arange(rows, dtype=jnp.int32)[:, None]
    piece = row // (half // 2)
    first, second = order[2 * blk] * span, order[2 * blk + 1] * span
    position = (
        jnp.where(piece < 2, first, second)
        + half * (piece % 2)
        + (half // 2) * co
        + row % (half // 2)
    )
    cosine, sine = tables(position)
    fresh_cosine, fresh_sine = tables(jnp.full((8 * each, 1), seq, jnp.int32))
    q_cols, kv_cols = w_query.shape[1] // 2, 2 * HEAD_DIM
    weights = (w_query, w_key, w_value)

    def projected(pieces, n, asks=()):
        joint = not asks
        size = half // 2 * n
        if joint:
            cols = q_cols + kv_cols
            shapes = [arr(size, cols), arr(size, cols), arr(size, 2 * cols)]
        else:
            shapes = [arr(size, kv_cols), arr(size, kv_cols), arr(size, 2 * kv_cols)]
            shapes += [arr(size + 16, q_cols), arr(size + 16, q_cols), arr(size + 16, 2 * q_cols)]

        def kernel(*refs):
            project_kernel(len(pieces), len(asks), joint, *refs)

        return call(
            kernel,
            shapes,
            (ids, *pieces, *asks, *weights),
            1,
            [pltpu.VMEM((width, 2 * kv_cols), BF16)],
            flops=4 * size * width * 2 * (q_cols + kv_cols),
            name="project",
        )

    def summed(near, far, peer, after=None):
        arrived = shift(peer, "co", 1)
        far = far + arrived[:, far.shape[1] :]
        if after is not None:
            far, _ = lax.optimization_barrier((far, after))
        return near, arrived, shift(far, "yh", 1)

    cut = half // 2
    low = shift(hidden, "tp", 1)
    high = shift(hidden, "tp", -1)
    far_a = shift(low[:cut], "tp", 1)
    far_b = shift(high[cut:], "tp", -1)
    own_asks = jnp.pad(lax.dynamic_slice_in_dim(asking, each * blk, each, 0), ((0, 16 - each), (0, 0)))
    asks = (own_asks, shift(own_asks, "tp", -1), shift(own_asks, "tp", 1), shift(own_asks, "tp", 2))
    phase_a = summed(*projected((hidden,), 1))
    phase_b = summed(*projected((high, low), 2))
    *kv_c, q_near, q_far, q_peer = projected((far_a, far_b), 1, asks)
    kv_c = summed(*kv_c)
    q_c = summed(q_near, q_far, q_peer, kv_c[2])

    kv = call(
        kv_kernel,
        arr(2, rows, HEAD_DIM, dtype=BF16),
        (ids, *phase_a, *phase_b, *kv_c, cosine, sine),
        1,
        [pltpu.VMEM((rows, HEAD_DIM), F32)],
        name="kv_rope",
    )
    unit = call(pair_kernel, arr(2, 2, rows, HEAD_DIM, dtype=BF16), (kv, shift(kv, "yl", 1)), name="pair")
    doc = 4 * rows
    queries, late = call(
        q_kernel,
        [arr(HEAD_DIM, doc, dtype=BF16), arr(HEAD_DIM, 256, dtype=BF16)],
        (ids, *phase_a, *phase_b, *q_c, cosine, sine, fresh_cosine, fresh_sine),
        1,
        name="q_rope",
    )
    queries = call(
        q_pair_kernel,
        arr(HEAD_DIM, 2 * doc + 256, dtype=BF16),
        (ids, queries, shift(queries, "co", 1), late),
        1,
        name="q_pair",
    )

    def attended(arrays, state, origins, split=False, lanes=None):
        return attend(ids, order, queries, arrays, state, origins, (zs, yls, 2 * doc // TILE), split, lanes)

    def origin(*steps):
        return [(dz, flip) for dz in steps for flip in range(2)]

    n = zs // 2
    ups, downs = [unit], [unit]
    state = None
    for step in range(1, n + 1):
        up, down = ups[-1], downs[-1]
        if step > 2:
            done = step - 3
            arrays = [unit] if done == 0 else [ups[done], downs[done]]
            state = attended(arrays, state, origin(*((0,) if done == 0 else (-done, done))))
            state, up, down = lax.optimization_barrier((state, up, down))
        if step == n:
            up, down = up[0], down[1]
        ups.append(shift(up, "z", 1))
        downs.append(shift(down, "z", -1))
    for done in range(n - 2, n):
        state = attended([ups[done], downs[done]], state, origin(-done, done))
    last, last_origin = [ups[n], downs[n]], origin(n)

    asked = attended(last, state, last_origin, True, (2 * doc, 256))
    asked_other = shift(asked[:, 128:], "co", 1)
    theirs = attended(last, state, last_origin, True, (doc, doc))
    doc_other = shift(theirs, "co", 1)
    kept, sent = call(
        merge_asked_kernel,
        [arr(16, 4 * HEAD_DIM, dtype=BF16)] * 2,
        (ids, asked, asked_other),
        1,
        name="merge_asked",
    )

    def whole(kept, sent):
        came = shift(sent, "yh", 1)
        return jnp.where(
            yh == 0, jnp.concatenate([kept, came], 1), jnp.concatenate([came, kept], 1)
        )

    answer = whole(kept, sent)[:each]
    decoded = lax.all_to_all(
        jnp.broadcast_to(answer[None], (zs * yls, *answer.shape)), BLK, 0, 0, tiled=True
    ).reshape(zs * yls * each, -1)
    ours = attended(last, state, last_origin, True, (0, doc))
    kept, sent = call(
        merge_kernel,
        [arr(half, 4 * HEAD_DIM, dtype=BF16)] * 2,
        (ids, ours, doc_other),
        1,
        [pltpu.VMEM((2, half, 4 * HEAD_DIM), BF16)],
        name="merge",
    )
    return whole(kept, sent), decoded


def solution(mesh):
    n_blk, n_tp, n_qg = (mesh.shape[a] for a in ("blk", "tp", "qg"))
    finer = Mesh(
        mesh.devices.reshape(n_blk // 2, 2, n_tp, n_qg // 2, 2), ("z", "yl", "tp", "yh", "co")
    )
    qg = ("yh", "co")
    return jax.shard_map(
        body,
        mesh=finer,
        in_specs=(P(("z", "yl", "tp"), qg), P("tp", qg), P(qg, "tp"), P(qg, "tp"), P(qg, "tp"), P()),
        out_specs=(P(("z", "yl", "yh", "co"), "tp"), P(qg, "tp")),
        check_vma=False,
    )
```
